256 devices in a mesh: dp: 8 (over z), vocab: 32 (over x, y, core).
Axes of the slice: x: 4, y: 4, z: 8, core: 2. Of those that a mesh axis runs over, the one named last changes fastest.
Arguments:
- hidden: bfloat16 [8, 2, 64, 4608], P('dp'), may hold values from -6 to 6
- table: bfloat16 [73728, 4608], P('vocab', 'dp'), may hold values from -0.25 to 0.25
- new_mask: int32 [73728], P('vocab'), may hold values from 0 to 1, as said below
- labels: int32 [8, 2, 64], P('dp'), may hold values from 0 to 73727
- in_grad: bfloat16 [8, 2, 768, 4608], P('dp', None, 'vocab'), may hold values from -0.75 to 0.75
- item_owner: int32 [8, 2, 768, 1], P('dp', None, 'vocab'), may hold values from 0 to 31; in each aligned block of 24 rows (0 to 23, 24 to 47, ..., all dimensions but the last counted through in order) at most 2 rows name the same one
- item_slot: int32 [8, 2, 768], P('dp', None, 'vocab'), may hold values from 0 to 255
- first_moment: float32 [8192, 4608], P('vocab', 'dp'), may hold values from -0.75 to 0.75
- second_moment: float32 [8192, 4608], P('vocab', 'dp'), may hold values from 0.0001 to 0.01
Outputs:
- token_loss: float32 [8, 2, 64], P('dp')
- d_hidden: bfloat16 [8, 2, 64, 4608], P('dp', None, None, 'vocab')
- update: float32 [8192, 4608], P('vocab', 'dp')
- first_out: float32 [8192, 4608], P('vocab', 'dp')
- second_out: float32 [8192, 4608], P('vocab', 'dp')
The draws below stay inside these ranges and needn't reach their ends.
Inputs may be any that keep to these rules, and one draw needn't show every extreme that they name: `new_mask`: each aligned block of 2304 entries holds exactly 256 ones. `item_owner`: within the 24 rows of one device in one block, no shard is named more than 2 times, a bound that some block reaches.
All inputs are finite; a program needn't handle non-finite values.
Results may differ from the reference program's by a relative error of at most 0.006.
Values may be sent and summed in bfloat16 or wider, within the bound.
No kernel may reach another device: no remote copies, remote signals or barrier semaphores. Data moves between devices by JAX's collectives and lax.ppermute only.
A program may use at most 128 MiB of HBM per device.

```python
import math
import jax
import jax.numpy as jnp
import numpy as np
from jax import lax

D = 4608
VOCAB_DEV = 2304
NEW_DEV = 256
SPAN = 64
SPANS = 2
ITEMS_DEV = 24
CAP = 2
VOCAB = 73728
NEW_ROWS = 8192
ITEMS = 768
N_DP = 8
N_VOCAB = 32


def draw_new_mask(key, part):
    shards = VOCAB // VOCAB_DEV
    keys = jax.random.split(jax.random.fold_in(key, 17), shards)
    orders = jax.vmap(lambda single: jax.random.permutation(single, VOCAB_DEV))(keys)
    return (orders < NEW_DEV).astype(jnp.int32).reshape(-1)


def place_ends(array, key, least, largest):
    spot = [jax.random.randint(jax.random.fold_in(key, axis), (), 0, length) for axis, length in enumerate(array.shape)]
    widest = array.shape.index(max(array.shape))
    next_to = spot[:widest] + [(spot[widest] + 1) % array.shape[widest]] + spot[widest + 1:]
    return array.at[tuple(spot)].set(least).at[tuple(next_to)].set(largest)


def steps_of(stream_key, extent, cuts, smallest, largest):
    level, own = 1.0, jax.random.fold_in(stream_key, 6)
    for position, blocks in cuts:
        steps = jnp.exp(jax.random.uniform(jax.random.fold_in(own, position), (blocks,), jnp.float32, smallest / len(cuts), largest / len(cuts)))
        level = level * jnp.repeat(steps, extent[position] // blocks).reshape([-1 if axis == position else 1 for axis in range(len(extent))])
    return level


def wide_ids(rng, shape, amount, skew):
    weights = [min(1 << octave, amount + 1 - (1 << octave)) * (1 << 20) // math.isqrt((1 << octave) ** skew) + 1 for octave in range((amount + 1).bit_length()) if 1 << octave <= amount]
    width = 1 + sum(weights) // (1 << 30)
    grid = np.cumsum(np.array([max(1, weight // width) for weight in weights]))
    lot = jax.random.randint(jax.random.fold_in(rng, 1), shape, 0, int(grid[len(weights) - 1]))
    start = jnp.left_shift(1, jnp.searchsorted(jnp.asarray(grid, jnp.int32), lot, side="right").astype(jnp.int32))
    rank = start - 1 + jax.random.randint(jax.random.fold_in(rng, 4), shape, 0, 1 << 30) % jnp.minimum(start, amount + 1 - start)
    return jax.random.permutation(jax.random.fold_in(rng, 2), amount)[rank].astype(jnp.int32)


def assign_block(stream_key, own, number, rows, number_of, top, bound, skew):
    order = jax.random.permutation(stream_key, number_of)
    crowded, common = portions_of(number_of, rows * top, bound, skew, True), portions_of(number_of, rows * top, bound, skew, False)
    places = jnp.arange(number_of)

    def named(sizes, rotation):
        used = int((sizes > 0).sum())
        fixed = max(1, used // 4)
        shifted = fixed + (places - fixed + rotation * (used - fixed)) % max(1, number_of - fixed)
        return jnp.zeros((number_of,), jnp.int32).at[order[jnp.where(places < fixed, places, shifted)]].set(jnp.asarray(sizes, jnp.int32))

    sizes = jnp.where(number % 4 == 0, named(crowded, number // 4), named(common, number - number // 4 - 1))
    mixed = jax.random.permutation(jax.random.fold_in(own, 3), number_of)
    donor, taker = mixed[0:number_of // 2 * 2:2], mixed[1:number_of // 2 * 2:2]
    room = jnp.minimum(sizes[donor] - 1, bound - sizes[taker]) // 2
    room = jnp.where((donor == order[0]) | (taker == order[0]) | (sizes[taker] == 0), 0, jnp.maximum(room, 0))
    shifted = jax.random.randint(jax.random.fold_in(own, 4), (number_of // 2,), 0, 1 << 20) % (room + 1)
    sizes = sizes.at[donor].add(-shifted).at[taker].add(shifted)
    members = jnp.searchsorted(jnp.cumsum(sizes), jnp.arange(rows * top), side="right").astype(jnp.int32)
    grid = members.reshape(top, rows).T
    grid = grid[jax.random.permutation(jax.random.fold_in(own, 1), rows)]
    rotation = jax.random.randint(jax.random.fold_in(own, 2), (rows, 1), 0, top)
    return jnp.take_along_axis(grid, (jnp.arange(top)[None, :] + rotation) % top, axis=1)


def portions_of(amount, total, bound, skew, full):
    weights = [(1 << 20) // math.isqrt(standing ** skew) + 1 for standing in range(1, amount + 1)]
    largest = bound if full else min(bound, max(-(-total // amount), total * weights[0] // sum(weights)))
    least = 1 if total - largest >= amount - 1 else 0
    holding, surplus = [largest] + [least] * (amount - 1), total - largest - least * (amount - 1)
    while surplus > 0:
        candidates = [i for i in range(1, amount) if holding[i] < largest] or [i for i in range(1, amount) if holding[i] < bound]
        whole, left = sum([weights[i] for i in candidates]), surplus
        for i in candidates:
            extra = min(bound - holding[i], max(1, left * weights[i] // whole), surplus)
            holding[i] = holding[i] + extra
            surplus = surplus - extra
    return np.array(holding)


def bell_draw(key, dims, spread, limit, cuts=(), kind=jnp.bfloat16):
    level = steps_of(key, dims, cuts, -0.22, 0.18) if cuts else 1.0
    values = jax.random.normal(key, dims, jnp.float32) * spread * level
    return jnp.minimum(jnp.maximum(values, -limit), limit).astype(kind)


def setup_inputs(seed: int = 0) -> dict:
    streams_of = jax.random.split(jax.random.key(seed), 10)
    hidden = bell_draw(streams_of[0], (N_DP, SPANS, SPAN, D), 1.0, 6.0, ((0, 8),))
    table = bell_draw(streams_of[1], (VOCAB, D), (D // 9) ** -0.5, 0.25, ((0, 32), (1, 8)))
    new_mask = draw_new_mask(jax.random.fold_in(streams_of[9], 71), 0)
    labels = place_ends(wide_ids(streams_of[3], (N_DP, SPANS, SPAN), VOCAB, 2), jax.random.fold_in(streams_of[3], 3), 0, VOCAB - 1).astype(jnp.int32)
    in_grad = bell_draw(streams_of[4], (N_DP, SPANS, ITEMS, D), 0.05, 0.75, ((0, 8), (2, 32)))
    item_owner_keys = jax.random.split(jax.random.fold_in(streams_of[5], 1), N_DP * SPANS * ITEMS // ITEMS_DEV)
    item_owner_turns = jax.random.permutation(jax.random.fold_in(streams_of[5], 3), N_DP * SPANS * ITEMS // ITEMS_DEV)
    item_owner = jax.vmap(lambda own, number: assign_block(jax.random.fold_in(streams_of[5], 2), own, number, ITEMS_DEV, N_VOCAB, 1, CAP, 2))(item_owner_keys, item_owner_turns).reshape((N_DP, SPANS, ITEMS, 1))
    item_slot = place_ends(jax.random.randint(streams_of[6], (N_DP, SPANS, ITEMS), 0, NEW_DEV), jax.random.fold_in(streams_of[6], 1), 0, NEW_DEV - 1).astype(jnp.int32)
    first_moment = bell_draw(streams_of[7], (NEW_ROWS, D), 0.05, 0.75, ((0, 32), (1, 8)), jnp.float32)
    second_moment = jnp.clip(jnp.exp(math.log(0.01) - 4.6051702 * jax.random.uniform(streams_of[8], (NEW_ROWS, D), jnp.float32) ** steps_of(streams_of[8], (NEW_ROWS, D), ((0, 32), (1, 8)), -0.2, 0.2)), 0.0001, 0.01)
    return {"hidden": hidden, "table": table, "new_mask": new_mask, "labels": labels, "in_grad": in_grad, "item_owner": item_owner, "item_slot": item_slot, "first_moment": first_moment, "second_moment": second_moment}


cap_value = 30.0
beta_one = 0.9
beta_two = 0.95
step_count = 10
epsilon = 1e-08
decay_rate = 0.1

def reference(hidden, table, new_mask, labels, in_grad, item_owner, item_slot, first_moment, second_moment):
    shards = new_mask.shape[0] // VOCAB_DEV
    order = jnp.argsort(1 - new_mask.reshape(shards, VOCAB_DEV), axis=1, stable=True)[:, :NEW_DEV].astype(jnp.int32)
    offsets = (jnp.arange(shards, dtype=jnp.int32) * VOCAB_DEV)[:, None]
    new_index = (order + offsets).reshape(-1).astype(jnp.int32)
    flat_hidden = hidden.reshape(-1, SPAN, D)
    flat_labels = labels.reshape(-1, SPAN)
    vocab_rows = table.shape[0]

    def one_block(carry, inputs):
        states, label_row = inputs
        raw = lax.dot_general(states, table, (((1,), (1,)), ((), ())), preferred_element_type=jnp.float32)
        capped = cap_value * jnp.tanh(raw / cap_value)
        expd = jnp.exp(capped)
        total = lax.optimization_barrier(jnp.sum(expd, axis=1))
        hits = jnp.arange(vocab_rows, dtype=jnp.int32)[None, :] == label_row[:, None]
        picked = lax.optimization_barrier(jnp.sum(jnp.where(hits, capped, 0.0), axis=1))
        loss = jnp.log(total) - picked
        error = ((expd / total[:, None] - hits.astype(jnp.float32)) * (1.0 - (capped / cap_value) ** 2)).astype(jnp.bfloat16)
        dstate = jnp.dot(error, table, preferred_element_type=jnp.float32).astype(jnp.bfloat16)
        chosen = error[:, new_index]
        carry = carry + jnp.dot(chosen.T, states, preferred_element_type=jnp.float32)
        return (carry, (loss, dstate))
    start = jnp.zeros((new_index.shape[0], D), jnp.float32)
    grads, (losses, dstates) = lax.scan(one_block, start, (flat_hidden, flat_labels))
    rows = in_grad.reshape(-1, D).astype(jnp.float32)
    targets = (item_owner.reshape(-1) * NEW_DEV + item_slot.reshape(-1)).astype(jnp.int32)
    grads = grads + jax.ops.segment_sum(rows, targets, num_segments=new_index.shape[0])
    params = table[new_index].astype(jnp.float32)
    first_out = beta_one * first_moment + (1.0 - beta_one) * grads
    second_out = beta_two * second_moment + (1.0 - beta_two) * grads * grads
    update = first_out / (1.0 - beta_one ** step_count) / (jnp.sqrt(second_out / (1.0 - beta_two ** step_count)) + epsilon) + decay_rate * params
    return (losses.reshape(labels.shape), dstates.reshape(hidden.shape), update, first_out, second_out)
```

```python
import jax
import jax.numpy as jnp
from jax import lax
from jax.sharding import PartitionSpec as P

cap_value = 30.0
beta_one = 0.9
beta_two = 0.95
step_count = 10
epsilon = 1e-08
decay_rate = 0.1


def sent_to_all(array, axis):
    peers = lax.axis_size(axis)
    return lax.all_to_all(
        jnp.broadcast_to(array[None], (peers, *array.shape)), axis, 0, 0, tiled=True
    )


def exchanged(parts, axis):
    return lax.all_to_all(parts, axis, split_axis=0, concat_axis=0, tiled=True)


def select_rows(new_mask, new_count):
    ranked = jnp.cumsum(new_mask) - 1
    wanted = (ranked[None, :] == jnp.arange(new_count, dtype=jnp.int32)[:, None]) & (
        new_mask[None, :] == 1
    )
    return wanted.astype(jnp.bfloat16)


def pack_items(rows, owner, slot, shards, capacity):
    onehot = (owner[:, None] == jnp.arange(shards, dtype=jnp.int32)[None, :]).astype(jnp.int32)
    running = jnp.cumsum(onehot, axis=0)
    ranked = jnp.sum(onehot * running, axis=1) - 1
    place = owner * capacity + ranked
    placing = jnp.arange(shards * capacity, dtype=jnp.int32)[:, None] == place[None, :]
    sent = jnp.dot(placing.astype(jnp.bfloat16), rows, preferred_element_type=jnp.float32).astype(
        jnp.bfloat16
    )
    targets = jnp.sum(placing.astype(jnp.int32) * (slot + 1)[None, :], axis=1) - 1
    return (sent.reshape(shards, capacity, rows.shape[1]), targets.reshape(shards, capacity))


def body(
    hidden, table, new_mask, labels, in_grad, item_owner, item_slot, first_moment, second_moment
):
    blocks, span, width = hidden.shape[1:]
    tokens = blocks * span
    new_count = first_moment.shape[0]
    rows, columns = table.shape
    groups = lax.axis_size("dp")
    shards = lax.axis_size("vocab")
    group = lax.axis_index("dp")
    shard = lax.axis_index("vocab")
    piece = width // shards
    total_tokens = groups * tokens
    row_part = rows // groups
    items_here = in_grad.shape[2]
    capacity = max(2, (2 * items_here + shards - 1) // shards)

    own = lax.dynamic_slice(
        hidden[0].reshape(tokens, width), (0, shard * piece), (tokens, piece)
    ).T
    slices = sent_to_all(own, "dp").transpose(1, 0, 2).reshape(piece, total_tokens)
    states = lax.all_gather(slices, "vocab", axis=0, tiled=True)
    label_row = sent_to_all(labels[0].reshape(tokens), "dp").reshape(total_tokens)

    whole = exchanged(table.reshape(groups, row_part, columns), "dp")
    whole = whole.transpose(1, 0, 2).reshape(row_part, width)

    raw = jnp.dot(whole, states, preferred_element_type=jnp.float32)
    squashed = jnp.tanh(raw / cap_value)
    capped = cap_value * squashed
    expd = jnp.exp(capped)
    row_ids = shard * rows + group * row_part + jnp.arange(row_part, dtype=jnp.int32)
    hits = row_ids[:, None] == label_row[None, :]
    local_total = jnp.sum(expd, axis=0)
    local_pick = jnp.sum(jnp.where(hits, capped, 0.0), axis=0)
    weights = (expd * (1.0 - squashed * squashed)).astype(jnp.bfloat16)
    all_weights = lax.all_gather(weights, "dp", axis=0, tiled=True)

    sums = jnp.concatenate([local_total, local_pick]).reshape(-1, tokens)
    sums = sent_to_all(sums, "vocab").sum(axis=0)
    sums = sent_to_all(sums, "dp").sum(axis=0).reshape(2, total_tokens)
    total, picked = sums[0], sums[1]
    loss = lax.dynamic_slice(
        (jnp.log(total) - picked).reshape(groups, tokens), (group, 0), (1, tokens)
    )
    inverse = 1.0 / total
    label_weight = (
        (jnp.exp(picked) - total) * (1.0 - (picked / cap_value) ** 2)
    ).astype(jnp.bfloat16)
    shard_rows = shard * rows + jnp.arange(rows, dtype=jnp.int32)
    error = jnp.where(
        shard_rows[:, None] == label_row[None, :], label_weight[None, :], all_weights
    )

    partial_states = (
        lax.dot_general(
            table, error, (((0,), (0,)), ((), ())), preferred_element_type=jnp.float32
        )
        * inverse[None, :]
    )
    split = shards // groups
    parts = (
        partial_states.reshape(split, columns // split, groups, tokens)
        .transpose(2, 0, 1, 3)
        .reshape(shards, columns // split, tokens)
    )
    d_states = exchanged(parts, "vocab").sum(axis=0).astype(jnp.bfloat16)
    d_states = lax.ppermute(
        d_states,
        ("dp", "vocab"),
        [
            (z * shards + g * split + s, g * shards + z * split + s)
            for z in range(groups)
            for g in range(groups)
            for s in range(split)
        ],
    )
    d_hidden = d_states.T.reshape(1, blocks, span, columns // split)

    sent_rows = []
    sent_targets = []
    for c in range(blocks):
        block_rows, block_targets = pack_items(
            in_grad[0, c], item_owner[0, c, :, 0], item_slot[0, c], shards, capacity
        )
        sent_rows.append(block_rows)
        sent_targets.append(block_targets)
    got_rows = exchanged(jnp.concatenate(sent_rows, axis=1), "vocab")
    got_targets = exchanged(jnp.concatenate(sent_targets, axis=1), "vocab")
    held = shards * blocks * capacity
    got_rows = got_rows.reshape(held, width).T.reshape(groups, columns, held)
    item_rows = exchanged(got_rows, "dp")
    item_targets = sent_to_all(got_targets.reshape(held), "dp")

    select = select_rows(new_mask, new_count)
    params = jnp.dot(select, table, preferred_element_type=jnp.float32)
    chosen = (
        jnp.dot(select, error, preferred_element_type=jnp.float32) * inverse[None, :]
    ).astype(jnp.bfloat16)
    own_states = lax.dynamic_slice(states, (group * columns, 0), (columns, total_tokens))
    grads = lax.dot_general(
        chosen, own_states, (((1,), (1,)), ((), ())), preferred_element_type=jnp.float32
    )
    picking = (
        jnp.arange(new_count, dtype=jnp.int32)[:, None] == item_targets.reshape(1, -1)
    ).astype(jnp.bfloat16)
    grads = grads + lax.dot_general(
        picking,
        item_rows.transpose(1, 0, 2).reshape(columns, groups * held),
        (((1,), (1,)), ((), ())),
        preferred_element_type=jnp.float32,
    )
    first_out = beta_one * first_moment + (1.0 - beta_one) * grads
    second_out = beta_two * second_moment + (1.0 - beta_two) * grads * grads
    update = (
        first_out
        / (1.0 - beta_one**step_count)
        / (jnp.sqrt(second_out / (1.0 - beta_two**step_count)) + epsilon)
        + decay_rate * params
    )
    return (loss.reshape(1, blocks, span), d_hidden, update, first_out, second_out)


def solution(mesh):
    return jax.shard_map(
        body,
        mesh=mesh,
        in_specs=(
            P("dp", None, None, None),
            P("vocab", "dp"),
            P("vocab"),
            P("dp", None, None),
            P("dp", None, "vocab", None),
            P("dp", None, "vocab", None),
            P("dp", None, "vocab"),
            P("vocab", "dp"),
            P("vocab", "dp"),
        ),
        out_specs=(
            P("dp", None, None),
            P("dp", None, None, "vocab"),
            P("vocab", "dp"),
            P("vocab", "dp"),
            P("vocab", "dp"),
        ),
        check_vma=False,
    )
```

```python
import jax
import jax.numpy as jnp
from jax import lax
from jax.experimental import pallas as pl
from jax.experimental.pallas import tpu as pltpu
from jax.sharding import PartitionSpec as P

cap_value = 30.0
beta_one = 0.9
beta_two = 0.95
step_count = 10
epsilon = 1e-08
decay_rate = 0.1


def sent_to_all(array, axis):
    peers = lax.axis_size(axis)
    return lax.all_to_all(
        jnp.broadcast_to(array[None], (peers, *array.shape)), axis, 0, 0, tiled=True
    )


def exchanged(parts, axis):
    return lax.all_to_all(parts, axis, split_axis=0, concat_axis=0, tiled=True)


def as_digits(numbers):
    return jnp.stack([numbers & 255, (numbers >> 8) & 255, numbers >> 16]).astype(jnp.bfloat16)


def from_digits(digits):
    low, middle, high = (digits[k].astype(jnp.int32) for k in range(3))
    return low + (middle << 8) + (high << 16)


def forward_kernel(first_row_ref, part_ref, states_ref, label_ref, weight_ref, sums_ref, raw_ref):
    step = pl.program_id(0)
    product = jnp.dot(part_ref[0], states_ref[...], preferred_element_type=jnp.float32)

    @pl.when(step == 0)
    def _():
        raw_ref[...] = product

    @pl.when(step > 0)
    def _():
        raw_ref[...] += product

    @pl.when(step == pl.num_programs(0) - 1)
    def _():
        rows, tokens = raw_ref.shape
        strip = 16
        labels = label_ref[...]

        def one_strip(k, carry):
            total, pick = carry
            at = pl.ds(pl.multiple_of(k * strip, strip), strip)
            squashed = jnp.tanh(raw_ref[at, :] * (1.0 / cap_value))
            capped = cap_value * squashed
            expd = jnp.exp(capped)
            ids = (
                lax.broadcasted_iota(jnp.int32, (strip, tokens), 0) + first_row_ref[0] + k * strip
            )
            weight_ref[at, :] = (expd * (1.0 - squashed * squashed)).astype(weight_ref.dtype)
            picked = jnp.where(ids == labels, capped, 0.0)
            for half in range(0, strip, 8):
                total = total + expd[half : half + 8]
                pick = pick + picked[half : half + 8]
            return total, pick

        zero = jnp.zeros((8, tokens), jnp.float32)
        total, pick = lax.fori_loop(0, rows // strip, one_strip, (zero, zero))
        sums_ref[0:1, :] = jnp.sum(total, axis=0, keepdims=True)
        sums_ref[1:2, :] = jnp.sum(pick, axis=0, keepdims=True)


def forward_block(whole, states, label_row, first_row):
    parts, rows, columns = whole.shape
    tokens = states.shape[1]
    return pl.pallas_call(
        forward_kernel,
        grid=(parts,),
        in_specs=[
            pl.BlockSpec(memory_space=pltpu.SMEM),
            pl.BlockSpec((1, rows, columns), lambda k: (k, 0, 0)),
            pl.BlockSpec((columns, tokens), lambda k: (k, 0)),
            pl.BlockSpec((1, tokens), lambda k: (0, 0)),
        ],
        out_specs=[
            pl.BlockSpec((rows, tokens), lambda k: (0, 0)),
            pl.BlockSpec((2, tokens), lambda k: (0, 0)),
        ],
        out_shape=[
            jax.ShapeDtypeStruct((rows, tokens), jnp.bfloat16),
            jax.ShapeDtypeStruct((2, tokens), jnp.float32),
        ],
        scratch_shapes=[pltpu.VMEM((rows, tokens), jnp.float32)],
        compiler_params=pltpu.CompilerParams(dimension_semantics=("arbitrary",)),
        cost_estimate=pl.CostEstimate(
            flops=2 * parts * rows * columns * tokens,
            bytes_accessed=2 * parts * columns * (rows + tokens),
            transcendentals=2 * rows * tokens,
        ),
        name="forward_block",
    )(first_row.reshape(1), whole, states, label_row.reshape(1, tokens))


def select_rows(new_mask, new_count):
    ranked = jnp.cumsum(new_mask) - 1
    wanted = (ranked[None, :] == jnp.arange(new_count, dtype=jnp.int32)[:, None]) & (
        new_mask[None, :] == 1
    )
    return wanted.astype(jnp.bfloat16)


def pack_items(rows, owner, slot, shards, capacity):
    onehot = (owner[:, None] == jnp.arange(shards, dtype=jnp.int32)[None, :]).astype(jnp.int32)
    running = jnp.cumsum(onehot, axis=0)
    ranked = jnp.sum(onehot * running, axis=1) - 1
    place = owner * capacity + ranked
    placing = jnp.arange(shards * capacity, dtype=jnp.int32)[:, None] == place[None, :]
    sent = jnp.dot(placing.astype(jnp.bfloat16), rows, preferred_element_type=jnp.float32).astype(
        jnp.bfloat16
    )
    codes = jnp.sum(placing.astype(jnp.int32) * (slot + 1)[None, :], axis=1)
    codes = jnp.broadcast_to(codes[:, None], (shards * capacity, 128)).astype(jnp.bfloat16)
    sent = jnp.concatenate([sent, codes], axis=1)
    return sent.reshape(shards, capacity, -1)


def body(
    hidden, table, new_mask, labels, in_grad, item_owner, item_slot, first_moment, second_moment
):
    blocks, span, width = hidden.shape[1:]
    tokens = blocks * span
    new_count = first_moment.shape[0]
    rows, columns = table.shape
    groups = lax.axis_size("dp")
    shards = lax.axis_size("vocab")
    group = lax.axis_index("dp")
    shard = lax.axis_index("vocab")
    piece = width // shards
    total_tokens = groups * tokens
    row_part = rows // groups
    items_here = in_grad.shape[2]
    capacity = max(2, (2 * items_here + shards - 1) // shards)

    own = lax.dynamic_slice(
        hidden[0].reshape(tokens, width), (0, shard * piece), (tokens, piece)
    ).T
    digits = jnp.pad(as_digits(labels[0].reshape(tokens)), ((0, 13), (0, 0)))
    arrived = sent_to_all(jnp.concatenate([own, digits], axis=0), "dp")
    slices = arrived[:, :piece].transpose(1, 0, 2).reshape(piece, total_tokens)
    states = lax.all_gather(slices, "vocab", axis=0, tiled=True)
    label_row = from_digits(arrived[:, piece : piece + 3].transpose(1, 0, 2)).reshape(total_tokens)

    whole = exchanged(table.reshape(groups, row_part, columns), "dp")

    packed = [
        pack_items(in_grad[0, c], item_owner[0, c, :, 0], item_slot[0, c], shards, capacity)
        for c in range(blocks)
    ]
    sent_rows = jnp.concatenate(packed, axis=1)
    whole, sent_rows = lax.optimization_barrier((whole, sent_rows))

    weights, local_sums = forward_block(
        whole, states, label_row, shard * rows + group * row_part
    )
    all_weights = lax.all_gather(weights, "dp", axis=0, tiled=True)

    sums = local_sums.reshape(-1, tokens)
    sums = sent_to_all(sums, "vocab").sum(axis=0)
    sums = sent_to_all(sums, "dp").sum(axis=0).reshape(2, total_tokens)
    total, picked = sums[0], sums[1]
    loss = lax.dynamic_slice(
        (jnp.log(total) - picked).reshape(groups, tokens), (group, 0), (1, tokens)
    )
    got_rows = exchanged(sent_rows, "vocab")
    held = shards * blocks * capacity
    got_rows = got_rows.reshape(held, width + 128).T
    item_parts = jnp.concatenate(
        [
            got_rows[:width].reshape(groups, columns, held),
            jnp.broadcast_to(got_rows[None, width : width + 16], (groups, 16, held)),
        ],
        axis=1,
    )

    inverse = 1.0 / total
    label_weight = (
        (jnp.exp(picked) - total) * (1.0 - (picked / cap_value) ** 2)
    ).astype(jnp.bfloat16)
    shard_rows = shard * rows + jnp.arange(rows, dtype=jnp.int32)
    error = jnp.where(
        shard_rows[:, None] == label_row[None, :], label_weight[None, :], all_weights
    )

    partial_states = (
        lax.dot_general(
            table, error, (((0,), (0,)), ((), ())), preferred_element_type=jnp.float32
        )
        * inverse[None, :]
    ).astype(jnp.bfloat16)
    item_parts, partial_states = lax.optimization_barrier((item_parts, partial_states))
    item_blocks = [lax.dynamic_index_in_dim(item_parts, group, 0, keepdims=False)]
    for away in range(1, groups):
        item_blocks.append(
            lax.ppermute(
                lax.dynamic_index_in_dim(
                    item_parts, lax.rem(group + away, groups), 0, keepdims=False
                ),
                "dp",
                [(k, (k + away) % groups) for k in range(groups)],
            )
        )
    item_block = jnp.concatenate(item_blocks, axis=1)
    split = shards // groups
    parts = (
        partial_states.reshape(split, columns // split, groups, tokens)
        .transpose(2, 0, 1, 3)
        .reshape(shards, columns // split, tokens)
    )
    d_states = exchanged(parts, "vocab").astype(jnp.float32).sum(axis=0).astype(jnp.bfloat16)
    d_states = lax.ppermute(
        d_states,
        ("dp", "vocab"),
        [
            (z * shards + g * split + s, g * shards + z * split + s)
            for z in range(groups)
            for g in range(groups)
            for s in range(split)
        ],
    )
    d_hidden = d_states.T.reshape(1, blocks, span, columns // split)

    select = select_rows(new_mask, new_count)
    params = jnp.dot(select, table, preferred_element_type=jnp.float32)
    chosen = (
        jnp.dot(select, error, preferred_element_type=jnp.float32) * inverse[None, :]
    ).astype(jnp.bfloat16)
    own_states = lax.dynamic_slice(states, (group * columns, 0), (columns, total_tokens))
    grads = lax.dot_general(
        chosen, own_states, (((1,), (1,)), ((), ())), preferred_element_type=jnp.float32
    )
    picking = (
        jnp.arange(new_count, dtype=jnp.int32)[:, None]
        == item_block[columns : columns + 1].astype(jnp.int32) - 1
    ).astype(jnp.bfloat16)
    grads = grads + lax.dot_general(
        picking,
        item_block[:columns],
        (((1,), (1,)), ((), ())),
        preferred_element_type=jnp.float32,
    )
    first_out = beta_one * first_moment + (1.0 - beta_one) * grads
    second_out = beta_two * second_moment + (1.0 - beta_two) * grads * grads
    update = (
        first_out
        / (1.0 - beta_one**step_count)
        / (jnp.sqrt(second_out / (1.0 - beta_two**step_count)) + epsilon)
        + decay_rate * params
    )
    return (loss.reshape(1, blocks, span), d_hidden, update, first_out, second_out)


def solution(mesh):
    return jax.shard_map(
        body,
        mesh=mesh,
        in_specs=(
            P("dp", None, None, None),
            P("vocab", "dp"),
            P("vocab"),
            P("dp", None, None),
            P("dp", None, "vocab", None),
            P("dp", None, "vocab", None),
            P("dp", None, "vocab"),
            P("vocab", "dp"),
            P("vocab", "dp"),
        ),
        out_specs=(
            P("dp", None, None),
            P("dp", None, None, "vocab"),
            P("vocab", "dp"),
            P("vocab", "dp"),
            P("vocab", "dp"),
        ),
        check_vma=False,
    )
```

```python
import jax
import jax.numpy as jnp
from jax import lax
from jax.experimental import pallas as pl
from jax.experimental.pallas import tpu as pltpu
from jax.sharding import PartitionSpec as P


cap_value = 30.0
beta_one = 0.9
beta_two = 0.95
step_count = 10
epsilon = 1e-08
decay_rate = 0.1


def sent_to_all(array, axis):
    peers = lax.axis_size(axis)
    return lax.all_to_all(
        jnp.broadcast_to(array[None], (peers, *array.shape)), axis, 0, 0, tiled=True
    )


def exchanged(parts, axis):
    return lax.all_to_all(parts, axis, split_axis=0, concat_axis=0, tiled=True)


def as_digits(numbers):
    return jnp.stack([numbers & 255, (numbers >> 8) & 255, numbers >> 16]).astype(jnp.bfloat16)


def from_digits(digits):
    low, middle, high = (digits[k].astype(jnp.int32) for k in range(3))
    return low + (middle << 8) + (high << 16)


def forward_kernel(first_row_ref, part_ref, states_ref, label_ref, weight_ref, sums_ref, raw_ref):
    step = pl.program_id(0)
    product = jnp.dot(part_ref[0], states_ref[...], preferred_element_type=jnp.float32)

    @pl.when(step == 0)
    def _():
        raw_ref[...] = product

    @pl.when(step > 0)
    def _():
        raw_ref[...] += product

    @pl.when(step == pl.num_programs(0) - 1)
    def _():
        rows, tokens = raw_ref.shape
        strip = 16
        labels = label_ref[...]

        def one_strip(k, carry):
            total, pick = carry
            at = pl.ds(pl.multiple_of(k * strip, strip), strip)
            squashed = jnp.tanh(raw_ref[at, :] * (1.0 / cap_value))
            capped = cap_value * squashed
            expd = jnp.exp(capped)
            ids = (
                lax.broadcasted_iota(jnp.int32, (strip, tokens), 0) + first_row_ref[0] + k * strip
            )
            weight_ref[at, :] = (expd * (1.0 - squashed * squashed)).astype(weight_ref.dtype)
            picked = jnp.where(ids == labels, capped, 0.0)
            for half in range(0, strip, 8):
                total = total + expd[half : half + 8]
                pick = pick + picked[half : half + 8]
            return total, pick

        zero = jnp.zeros((8, tokens), jnp.float32)
        total, pick = lax.fori_loop(0, rows // strip, one_strip, (zero, zero))
        sums_ref[0:1, :] = jnp.sum(total, axis=0, keepdims=True)
        sums_ref[1:2, :] = jnp.sum(pick, axis=0, keepdims=True)


def forward_block(whole, states, label_row, first_row):
    parts, rows, columns = whole.shape
    tokens = states.shape[1]
    return pl.pallas_call(
        forward_kernel,
        grid=(parts,),
        in_specs=[
            pl.BlockSpec(memory_space=pltpu.SMEM),
            pl.BlockSpec((1, rows, columns), lambda k: (k, 0, 0)),
            pl.BlockSpec((columns, tokens), lambda k: (k, 0)),
            pl.BlockSpec((1, tokens), lambda k: (0, 0)),
        ],
        out_specs=[
            pl.BlockSpec((rows, tokens), lambda k: (0, 0)),
            pl.BlockSpec((2, tokens), lambda k: (0, 0)),
        ],
        out_shape=[
            jax.ShapeDtypeStruct((rows, tokens), jnp.bfloat16),
            jax.ShapeDtypeStruct((2, tokens), jnp.float32),
        ],
        scratch_shapes=[pltpu.VMEM((rows, tokens), jnp.float32)],
        compiler_params=pltpu.CompilerParams(dimension_semantics=("arbitrary",)),
        cost_estimate=pl.CostEstimate(
            flops=2 * parts * rows * columns * tokens,
            bytes_accessed=2 * parts * columns * (rows + tokens),
            transcendentals=2 * rows * tokens,
        ),
        name="forward_block",
    )(first_row.reshape(1), whole, states, label_row.reshape(1, tokens))


def select_rows(new_mask, new_count):
    ranked = jnp.cumsum(new_mask) - 1
    wanted = (ranked[None, :] == jnp.arange(new_count, dtype=jnp.int32)[:, None]) & (
        new_mask[None, :] == 1
    )
    return wanted.astype(jnp.bfloat16)


def pack_items(arrived, columns, sets, shards, capacity):
    rows = arrived.reshape(-1, arrived.shape[2])
    owner = rows[:, columns].astype(jnp.int32).reshape(sets, -1)
    earlier = jnp.tril(jnp.ones((owner.shape[1], owner.shape[1]), jnp.bool_), -1)
    ranked = jnp.sum(
        ((owner[:, :, None] == owner[:, None, :]) & earlier[None]).astype(jnp.int32), axis=2
    )
    place = (owner * sets + jnp.arange(sets, dtype=jnp.int32)[:, None]) * capacity + ranked
    held = shards * sets * capacity
    placing = jnp.arange(held, dtype=jnp.int32)[:, None] == place.reshape(1, -1)
    sent = jnp.dot(placing.astype(jnp.bfloat16), rows, preferred_element_type=jnp.float32)
    return sent.astype(jnp.bfloat16).reshape(shards, sets * capacity, -1)


def body(
    hidden, table, new_mask, labels, in_grad, item_owner, item_slot, first_moment, second_moment
):
    blocks, span, width = hidden.shape[1:]
    tokens = blocks * span
    new_count = first_moment.shape[0]
    rows, columns = table.shape
    groups = lax.axis_size("dp")
    shards = lax.axis_size("vocab")
    group = lax.axis_index("dp")
    shard = lax.axis_index("vocab")
    piece = width // shards
    total_tokens = groups * tokens
    row_part = rows // groups
    items_here = in_grad.shape[2]
    capacity = max(2, (2 * items_here + shards - 1) // shards)

    own = lax.dynamic_slice(
        hidden[0].reshape(tokens, width), (0, shard * piece), (tokens, piece)
    ).T
    digits = jnp.pad(as_digits(labels[0].reshape(tokens)), ((0, 13), (0, 0)))
    arrived = sent_to_all(jnp.concatenate([own, digits], axis=0), "dp")
    slices = arrived[:, :piece].transpose(1, 0, 2).reshape(piece, total_tokens)
    states = lax.all_gather(slices, "vocab", axis=0, tiled=True)
    label_row = from_digits(arrived[:, piece : piece + 3].transpose(1, 0, 2)).reshape(total_tokens)

    whole = exchanged(table.reshape(groups, row_part, columns), "dp")

    items = blocks * items_here
    item_columns = in_grad[0].reshape(items, groups, columns).transpose(1, 0, 2)
    lane = jnp.arange(64, dtype=jnp.int32)[None, :]
    marks = jnp.where(
        lane == 0,
        item_owner[0].reshape(items, 1),
        jnp.where(lane == 1, item_slot[0].reshape(items, 1) + 1, 0),
    ).astype(jnp.bfloat16)
    item_columns = jnp.concatenate(
        [item_columns, jnp.broadcast_to(marks[None], (groups, items, 64))], axis=2
    )
    whole, item_columns = lax.optimization_barrier((whole, item_columns))

    weights, local_sums = forward_block(
        whole, states, label_row, shard * rows + group * row_part
    )
    all_weights = lax.all_gather(weights, "dp", axis=0, tiled=True)

    sums = local_sums.reshape(-1, tokens)
    sums = sent_to_all(sums, "vocab").sum(axis=0)
    sums = sent_to_all(sums, "dp").sum(axis=0).reshape(2, total_tokens)
    total, picked = sums[0], sums[1]
    loss = lax.dynamic_slice(
        (jnp.log(total) - picked).reshape(groups, tokens), (group, 0), (1, tokens)
    )
    item_columns = exchanged(item_columns, "dp")
    sent_rows = pack_items(item_columns, columns, groups * blocks, shards, capacity)
    got_rows = exchanged(sent_rows, "vocab").reshape(-1, columns + 64)
    targets = got_rows[:, columns + 1].astype(jnp.int32) - 1

    inverse = 1.0 / total
    label_weight = (
        (jnp.exp(picked) - total) * (1.0 - (picked / cap_value) ** 2)
    ).astype(jnp.bfloat16)
    shard_rows = shard * rows + jnp.arange(rows, dtype=jnp.int32)
    error = jnp.where(
        shard_rows[:, None] == label_row[None, :], label_weight[None, :], all_weights
    )

    partial_states = (
        lax.dot_general(
            table, error, (((0,), (0,)), ((), ())), preferred_element_type=jnp.float32
        )
        * inverse[None, :]
    ).astype(jnp.bfloat16)
    split = shards // groups
    parts = (
        partial_states.reshape(split, columns // split, groups, tokens)
        .transpose(2, 0, 1, 3)
        .reshape(shards, columns // split, tokens)
    )
    d_states = exchanged(parts, "vocab").astype(jnp.float32).sum(axis=0).astype(jnp.bfloat16)
    d_states = lax.ppermute(
        d_states,
        ("dp", "vocab"),
        [
            (z * shards + g * split + s, g * shards + z * split + s)
            for z in range(groups)
            for g in range(groups)
            for s in range(split)
        ],
    )
    d_hidden = d_states.T.reshape(1, blocks, span, columns // split)

    select = select_rows(new_mask, new_count)
    params = jnp.dot(select, table, preferred_element_type=jnp.float32)
    chosen = (
        jnp.dot(select, error, preferred_element_type=jnp.float32) * inverse[None, :]
    ).astype(jnp.bfloat16)
    own_states = lax.dynamic_slice(states, (group * columns, 0), (columns, total_tokens))
    grads = lax.dot_general(
        chosen, own_states, (((1,), (1,)), ((), ())), preferred_element_type=jnp.float32
    )
    picking = (jnp.arange(new_count, dtype=jnp.int32)[:, None] == targets[None, :]).astype(
        jnp.bfloat16
    )
    grads = grads + jnp.dot(
        picking, got_rows[:, :columns], preferred_element_type=jnp.float32
    )
    first_out = beta_one * first_moment + (1.0 - beta_one) * grads
    second_out = beta_two * second_moment + (1.0 - beta_two) * grads * grads
    update = (
        first_out
        / (1.0 - beta_one**step_count)
        / (jnp.sqrt(second_out / (1.0 - beta_two**step_count)) + epsilon)
        + decay_rate * params
    )
    return (loss.reshape(1, blocks, span), d_hidden, update, first_out, second_out)


def solution(mesh):
    return jax.shard_map(
        body,
        mesh=mesh,
        in_specs=(
            P("dp", None, None, None),
            P("vocab", "dp"),
            P("vocab"),
            P("dp", None, None),
            P("dp", None, "vocab", None),
            P("dp", None, "vocab", None),
            P("dp", None, "vocab"),
            P("vocab", "dp"),
            P("vocab", "dp"),
        ),
        out_specs=(
            P("dp", None, None),
            P("dp", None, None, "vocab"),
            P("vocab", "dp"),
            P("vocab", "dp"),
            P("vocab", "dp"),
        ),
        check_vma=False,
    )
```

```python
import jax
import jax.numpy as jnp
from jax import lax
from jax.experimental import pallas as pl
from jax.experimental.pallas import tpu as pltpu
from jax.sharding import PartitionSpec as P


cap_value = 30.0
beta_one = 0.9
beta_two = 0.95
step_count = 10
epsilon = 1e-08
decay_rate = 0.1


def sent_to_all(array, axis):
    peers = lax.axis_size(axis)
    return lax.all_to_all(
        jnp.broadcast_to(array[None], (peers, *array.shape)), axis, 0, 0, tiled=True
    )


def exchanged(parts, axis):
    return lax.all_to_all(parts, axis, split_axis=0, concat_axis=0, tiled=True)


def as_digits(numbers):
    return jnp.stack([numbers & 255, (numbers >> 8) & 255, numbers >> 16]).astype(jnp.bfloat16)


def from_digits(digits):
    low, middle, high = (digits[k].astype(jnp.int32) for k in range(3))
    return low + (middle << 8) + (high << 16)


def forward_kernel(place_ref, *refs):
    part_refs = refs[:-6]
    states_ref, label_ref, weight_ref, sums_ref, raw_ref, part_ref = refs[-6:]
    step = pl.program_id(0)
    rows, columns = part_ref.shape
    whole = columns // 128

    for k, packed_ref in enumerate(part_refs):

        @pl.when(step == k)
        def _(packed_ref=packed_ref):
            for at in range(whole):
                part_ref[:, at * 128 : (at + 1) * 128] = packed_ref[at * rows : (at + 1) * rows, :]
            rest = packed_ref[whole * rows :, :]
            part_ref[: rows // 2, whole * 128 :] = rest[:, :64]
            part_ref[rows // 2 :, whole * 128 :] = rest[:, 64:]

    product = jnp.dot(part_ref[...], states_ref[...], preferred_element_type=jnp.float32)

    @pl.when(step == 0)
    def _():
        raw_ref[...] = product

    @pl.when(step > 0)
    def _():
        raw_ref[...] += product

    @pl.when(step == pl.num_programs(0) - 1)
    def _():
        tokens = raw_ref.shape[1]
        strip = 16
        labels = label_ref[...]

        def one_strip(k, carry):
            total, pick = carry
            at = pl.ds(pl.multiple_of(k * strip, strip), strip)
            squashed = jnp.tanh(raw_ref[at, :] * (1.0 / cap_value))
            capped = cap_value * squashed
            expd = jnp.exp(capped)
            ids = (
                lax.broadcasted_iota(jnp.int32, (strip, tokens), 0) + place_ref[0] + k * strip
            )
            weight_ref[at, :] = (expd * (1.0 - squashed * squashed)).astype(weight_ref.dtype)
            picked = jnp.where(ids == labels, capped, 0.0)
            for half in range(0, strip, 8):
                total = total + expd[half : half + 8]
                pick = pick + picked[half : half + 8]
            return total, pick

        zero = jnp.zeros((8, tokens), jnp.float32)
        total, pick = lax.fori_loop(0, rows // strip, one_strip, (zero, zero))
        sums_ref[0:1, :] = jnp.sum(total, axis=0, keepdims=True)
        sums_ref[1:2, :] = jnp.sum(pick, axis=0, keepdims=True)


def forward_block(whole, states, label_row, first_row, group, columns):
    parts = len(whole)
    rows = whole[0].size // columns
    tokens = states.shape[1]
    return pl.pallas_call(
        forward_kernel,
        grid_spec=pltpu.PrefetchScalarGridSpec(
            num_scalar_prefetch=1,
            grid=(parts,),
            in_specs=[
                *[pl.BlockSpec(part.shape, lambda k, place: (0, 0)) for part in whole],
                pl.BlockSpec((columns, tokens), lambda k, place: ((place[1] - k) & (parts - 1), 0)),
                pl.BlockSpec((1, tokens), lambda k, place: (0, 0)),
            ],
            out_specs=[
                pl.BlockSpec((rows, tokens), lambda k, place: (0, 0)),
                pl.BlockSpec((2, tokens), lambda k, place: (0, 0)),
            ],
            scratch_shapes=[
                pltpu.VMEM((rows, tokens), jnp.float32),
                pltpu.VMEM((rows, columns), jnp.bfloat16),
            ],
        ),
        out_shape=[
            jax.ShapeDtypeStruct((rows, tokens), jnp.bfloat16),
            jax.ShapeDtypeStruct((2, tokens), jnp.float32),
        ],
        compiler_params=pltpu.CompilerParams(dimension_semantics=("arbitrary",)),
        cost_estimate=pl.CostEstimate(
            flops=2 * parts * rows * columns * tokens,
            bytes_accessed=2 * parts * columns * (rows + tokens),
            transcendentals=2 * rows * tokens,
        ),
        name="forward_block",
    )(jnp.stack([first_row, group]), *whole, states, label_row.reshape(1, tokens))


def spread(parts, axis):
    peers = len(parts)
    middle = peers // 2
    order = sorted(range(1, peers), key=lambda away: (abs(away - middle), away))
    came = {0: parts[0]}
    for away in order:
        came[away] = lax.ppermute(
            parts[away], axis, [(k, (k + away) % peers) for k in range(peers)]
        )
    return [came[k] for k in range(peers)]


def packing_kernel(group_ref, table_ref, *refs):
    part_refs, rows_ref = refs[:-1], refs[-1]
    columns, rows = table_ref.shape
    lanes = 128
    peers = len(part_refs)
    part = rows // peers
    whole = columns // lanes
    for at in range(0, rows, lanes):
        rows_ref[at : at + lanes, :] = table_ref[:, at : at + lanes].T
    for away in range(peers):
        first = pl.multiple_of(((group_ref[0] + away) & (peers - 1)) * part, part)
        for k in range(whole):
            part_refs[away][k * part : (k + 1) * part, :] = rows_ref[
                pl.ds(first, part), k * lanes : (k + 1) * lanes
            ]
        part_refs[away][whole * part :, :] = jnp.concatenate(
            [
                rows_ref[pl.ds(first, part // 2), whole * lanes :],
                rows_ref[pl.ds(first + part // 2, part // 2), whole * lanes :],
            ],
            axis=1,
        )


def packed_parts(table, group, peers):
    rows, columns = table.shape
    part = jax.ShapeDtypeStruct((rows * columns // peers // 128, 128), table.dtype)
    return pl.pallas_call(
        packing_kernel,
        in_specs=[
            pl.BlockSpec(memory_space=pltpu.SMEM),
            pl.BlockSpec(memory_space=pltpu.VMEM),
        ],
        out_specs=[pl.BlockSpec(memory_space=pltpu.VMEM)] * peers,
        out_shape=[part] * peers,
        scratch_shapes=[pltpu.VMEM((rows, columns), table.dtype)],
        cost_estimate=pl.CostEstimate(
            flops=rows * columns * 8, bytes_accessed=rows * columns * 4, transcendentals=0
        ),
        name="packed_parts",
    )(group.reshape(1), table.T)


def select_rows(new_mask, new_count):
    ranked = jnp.cumsum(new_mask) - 1
    wanted = (ranked[None, :] == jnp.arange(new_count, dtype=jnp.int32)[:, None]) & (
        new_mask[None, :] == 1
    )
    return wanted.astype(jnp.bfloat16)


def pack_items(arrived, columns, sets, shards, capacity):
    rows = arrived.reshape(-1, arrived.shape[2])
    owner = rows[:, columns].astype(jnp.int32).reshape(sets, -1)
    earlier = jnp.tril(jnp.ones((owner.shape[1], owner.shape[1]), jnp.bool_), -1)
    ranked = jnp.sum(
        ((owner[:, :, None] == owner[:, None, :]) & earlier[None]).astype(jnp.int32), axis=2
    )
    place = (owner * sets + jnp.arange(sets, dtype=jnp.int32)[:, None]) * capacity + ranked
    held = shards * sets * capacity
    placing = jnp.arange(held, dtype=jnp.int32)[:, None] == place.reshape(1, -1)
    sent = jnp.dot(placing.astype(jnp.bfloat16), rows, preferred_element_type=jnp.float32)
    return sent.astype(jnp.bfloat16).reshape(shards, sets * capacity, -1)


def body(
    hidden, table, new_mask, labels, in_grad, item_owner, item_slot, first_moment, second_moment
):
    blocks, span, width = hidden.shape[1:]
    tokens = blocks * span
    new_count = first_moment.shape[0]
    rows, columns = table.shape
    groups = lax.axis_size("dp")
    shards = lax.axis_size("vocab")
    group = lax.axis_index("dp")
    shard = lax.axis_index("vocab")
    piece = width // shards
    total_tokens = groups * tokens
    row_part = rows // groups
    items_here = in_grad.shape[2]
    capacity = max(2, (2 * items_here + shards - 1) // shards)

    own = lax.dynamic_slice(
        hidden[0].reshape(tokens, width), (0, shard * piece), (tokens, piece)
    ).T
    digits = jnp.pad(as_digits(labels[0].reshape(tokens)), ((0, 13), (0, 0)))
    arrived = sent_to_all(jnp.concatenate([own, digits], axis=0), "dp")
    slices = arrived[:, :piece].transpose(1, 0, 2).reshape(piece, total_tokens)
    states = lax.all_gather(slices, "vocab", axis=0, tiled=True)
    label_row = from_digits(arrived[:, piece : piece + 3].transpose(1, 0, 2)).reshape(total_tokens)

    prepared = packed_parts(table, group, groups)
    whole = spread(prepared, "dp")

    items = blocks * items_here
    item_columns = in_grad[0].reshape(items, groups, columns).transpose(1, 0, 2)
    lane = jnp.arange(64, dtype=jnp.int32)[None, :]
    marks = jnp.where(
        lane == 0,
        item_owner[0].reshape(items, 1),
        jnp.where(lane == 1, item_slot[0].reshape(items, 1) + 1, 0),
    ).astype(jnp.bfloat16)
    item_columns = jnp.concatenate(
        [item_columns, jnp.broadcast_to(marks[None], (groups, items, 64))], axis=2
    )
    item_columns = exchanged(item_columns, "dp")

    weights, local_sums = forward_block(
        whole, states, label_row, shard * rows + group * row_part, group, columns
    )
    all_weights = lax.all_gather(weights, "dp", axis=0, tiled=True)

    sums = local_sums.reshape(-1, tokens)
    sums = sent_to_all(sums, "vocab").sum(axis=0)
    sums = sent_to_all(sums, "dp").sum(axis=0).reshape(2, total_tokens)
    total, picked = sums[0], sums[1]
    loss = lax.dynamic_slice(
        (jnp.log(total) - picked).reshape(groups, tokens), (group, 0), (1, tokens)
    )
    sent_rows = pack_items(item_columns, columns, groups * blocks, shards, capacity)
    got_rows = exchanged(sent_rows, "vocab").reshape(-1, columns + 64)
    targets = got_rows[:, columns + 1].astype(jnp.int32) - 1

    inverse = 1.0 / total
    label_weight = (
        (jnp.exp(picked) - total) * (1.0 - (picked / cap_value) ** 2)
    ).astype(jnp.bfloat16)
    shard_rows = shard * rows + jnp.arange(rows, dtype=jnp.int32)
    error = jnp.where(
        shard_rows[:, None] == label_row[None, :], label_weight[None, :], all_weights
    )

    partial_states = (
        lax.dot_general(
            table, error, (((0,), (0,)), ((), ())), preferred_element_type=jnp.float32
        )
        * inverse[None, :]
    ).astype(jnp.bfloat16)
    split = shards // groups
    parts = (
        partial_states.reshape(split, columns // split, groups, tokens)
        .transpose(2, 0, 1, 3)
        .reshape(shards, columns // split, tokens)
    )
    d_states = exchanged(parts, "vocab").astype(jnp.float32).sum(axis=0).astype(jnp.bfloat16)
    d_states = lax.ppermute(
        d_states,
        ("dp", "vocab"),
        [
            (z * shards + g * split + s, g * shards + z * split + s)
            for z in range(groups)
            for g in range(groups)
            for s in range(split)
        ],
    )
    d_hidden = d_states.T.reshape(1, blocks, span, columns // split)

    select = select_rows(new_mask, new_count)
    params = jnp.dot(select, table, preferred_element_type=jnp.float32)
    chosen = (
        jnp.dot(select, error, preferred_element_type=jnp.float32) * inverse[None, :]
    ).astype(jnp.bfloat16)
    own_states = lax.dynamic_slice(states, (group * columns, 0), (columns, total_tokens))
    grads = lax.dot_general(
        chosen, own_states, (((1,), (1,)), ((), ())), preferred_element_type=jnp.float32
    )
    picking = (jnp.arange(new_count, dtype=jnp.int32)[:, None] == targets[None, :]).astype(
        jnp.bfloat16
    )
    grads = grads + jnp.dot(
        picking, got_rows[:, :columns], preferred_element_type=jnp.float32
    )
    first_out = beta_one * first_moment + (1.0 - beta_one) * grads
    second_out = beta_two * second_moment + (1.0 - beta_two) * grads * grads
    update = (
        first_out
        / (1.0 - beta_one**step_count)
        / (jnp.sqrt(second_out / (1.0 - beta_two**step_count)) + epsilon)
        + decay_rate * params
    )
    return (loss.reshape(1, blocks, span), d_hidden, update, first_out, second_out)


def solution(mesh):
    return jax.shard_map(
        body,
        mesh=mesh,
        in_specs=(
            P("dp", None, None, None),
            P("vocab", "dp"),
            P("vocab"),
            P("dp", None, None),
            P("dp", None, "vocab", None),
            P("dp", None, "vocab", None),
            P("dp", None, "vocab"),
            P("vocab", "dp"),
            P("vocab", "dp"),
        ),
        out_specs=(
            P("dp", None, None),
            P("dp", None, None, "vocab"),
            P("vocab", "dp"),
            P("vocab", "dp"),
            P("vocab", "dp"),
        ),
        check_vma=False,
    )
```

```python
import jax
import jax.numpy as jnp
from jax import lax
from jax.experimental import pallas as pl
from jax.experimental.pallas import tpu as pltpu
from jax.sharding import PartitionSpec as P


cap_value = 30.0
beta_one = 0.9
beta_two = 0.95
step_count = 10
epsilon = 1e-08
decay_rate = 0.1


def sent_to_all(array, axis):
    peers = lax.axis_size(axis)
    return lax.all_to_all(
        jnp.broadcast_to(array[None], (peers, *array.shape)), axis, 0, 0, tiled=True
    )


def exchanged(parts, axis):
    return lax.all_to_all(parts, axis, split_axis=0, concat_axis=0, tiled=True)


def as_digits(numbers):
    return jnp.stack([numbers & 255, (numbers >> 8) & 255, numbers >> 16]).astype(jnp.bfloat16)


def from_digits(digits):
    low, middle, high = (digits[k].astype(jnp.int32) for k in range(3))
    return low + (middle << 8) + (high << 16)


def assembly_kernel(group_ref, *refs):
    part_refs, whole_ref, held_ref = refs[:-2], refs[-2], refs[-1]
    peers = len(part_refs)
    rows = whole_ref.shape[0]
    columns = whole_ref.shape[1] // peers
    full = columns // 128
    for k, part_ref in enumerate(part_refs):
        held_ref[k] = part_ref[...]
    for block in range(peers):
        source = (group_ref[0] - block) & (peers - 1)
        rest = held_ref[source, full * rows :, :]
        rest = jnp.concatenate([rest[:, :64], rest[:, 64:]], axis=0)
        pieces = [held_ref[source, k * rows : (k + 1) * rows, :] for k in range(full)]
        whole_ref[:, block * columns : (block + 1) * columns] = jnp.concatenate(
            [*pieces, rest], axis=1
        )


def assembled(parts, group, columns):
    peers = len(parts)
    rows = parts[0].size // columns
    return pl.pallas_call(
        assembly_kernel,
        in_specs=[
            pl.BlockSpec(memory_space=pltpu.SMEM),
            *[pl.BlockSpec(memory_space=pltpu.VMEM)] * peers,
        ],
        out_specs=pl.BlockSpec(memory_space=pltpu.VMEM),
        out_shape=jax.ShapeDtypeStruct((rows, columns * peers), parts[0].dtype),
        scratch_shapes=[pltpu.VMEM((peers, *parts[0].shape), parts[0].dtype)],
        cost_estimate=pl.CostEstimate(
            flops=rows * columns * peers * 8,
            bytes_accessed=rows * columns * peers * 4,
            transcendentals=0,
        ),
        name="assembled",
    )(group.reshape(1), *parts)


def spread(parts, axis):
    peers = len(parts)
    middle = peers // 2
    order = sorted(range(1, peers), key=lambda away: (abs(away - middle), away))
    came = {0: parts[0]}
    for away in order:
        came[away] = lax.ppermute(
            parts[away], axis, [(k, (k + away) % peers) for k in range(peers)]
        )
    return [came[k] for k in range(peers)]


def packing_kernel(group_ref, table_ref, *refs):
    part_refs, rows_ref = refs[:-1], refs[-1]
    columns, rows = table_ref.shape
    lanes = 128
    peers = len(part_refs)
    part = rows // peers
    whole = columns // lanes
    for at in range(0, rows, lanes):
        rows_ref[at : at + lanes, :] = table_ref[:, at : at + lanes].T
    for away in range(peers):
        first = pl.multiple_of(((group_ref[0] + away) & (peers - 1)) * part, part)
        for k in range(whole):
            part_refs[away][k * part : (k + 1) * part, :] = rows_ref[
                pl.ds(first, part), k * lanes : (k + 1) * lanes
            ]
        part_refs[away][whole * part :, :] = jnp.concatenate(
            [
                rows_ref[pl.ds(first, part // 2), whole * lanes :],
                rows_ref[pl.ds(first + part // 2, part // 2), whole * lanes :],
            ],
            axis=1,
        )


def packed_parts(table, group, peers):
    rows, columns = table.shape
    part = jax.ShapeDtypeStruct((rows * columns // peers // 128, 128), table.dtype)
    return pl.pallas_call(
        packing_kernel,
        in_specs=[
            pl.BlockSpec(memory_space=pltpu.SMEM),
            pl.BlockSpec(memory_space=pltpu.VMEM),
        ],
        out_specs=[pl.BlockSpec(memory_space=pltpu.VMEM)] * peers,
        out_shape=[part] * peers,
        scratch_shapes=[pltpu.VMEM((rows, columns), table.dtype)],
        cost_estimate=pl.CostEstimate(
            flops=rows * columns * 8, bytes_accessed=rows * columns * 4, transcendentals=0
        ),
        name="packed_parts",
    )(group.reshape(1), table.T)


def select_rows(new_mask, new_count):
    ranked = jnp.cumsum(new_mask) - 1
    wanted = (ranked[None, :] == jnp.arange(new_count, dtype=jnp.int32)[:, None]) & (
        new_mask[None, :] == 1
    )
    return wanted.astype(jnp.bfloat16)


def pack_items(arrived, columns, sets, shards, capacity):
    rows = arrived.reshape(-1, arrived.shape[2])
    owner = rows[:, columns].astype(jnp.int32).reshape(sets, -1)
    earlier = jnp.tril(jnp.ones((owner.shape[1], owner.shape[1]), jnp.bool_), -1)
    ranked = jnp.sum(
        ((owner[:, :, None] == owner[:, None, :]) & earlier[None]).astype(jnp.int32), axis=2
    )
    place = (owner * sets + jnp.arange(sets, dtype=jnp.int32)[:, None]) * capacity + ranked
    held = shards * sets * capacity
    placing = jnp.arange(held, dtype=jnp.int32)[:, None] == place.reshape(1, -1)
    sent = jnp.dot(placing.astype(jnp.bfloat16), rows, preferred_element_type=jnp.float32)
    return sent.astype(jnp.bfloat16).reshape(shards, sets * capacity, -1)


def body(
    hidden, table, new_mask, labels, in_grad, item_owner, item_slot, first_moment, second_moment
):
    blocks, span, width = hidden.shape[1:]
    tokens = blocks * span
    new_count = first_moment.shape[0]
    rows, columns = table.shape
    groups = lax.axis_size("dp")
    shards = lax.axis_size("vocab")
    group = lax.axis_index("dp")
    shard = lax.axis_index("vocab")
    piece = width // shards
    total_tokens = groups * tokens
    row_part = rows // groups
    items_here = in_grad.shape[2]
    capacity = max(2, (2 * items_here + shards - 1) // shards)

    own = lax.dynamic_slice(
        hidden[0].reshape(tokens, width), (0, shard * piece), (tokens, piece)
    ).T
    digits = jnp.pad(as_digits(labels[0].reshape(tokens)), ((0, 13), (0, 0)))
    arrived = sent_to_all(jnp.concatenate([own, digits], axis=0), "dp")
    slices = arrived[:, :piece].transpose(1, 0, 2).reshape(piece, total_tokens)
    states = lax.all_gather(slices, "vocab", axis=0, tiled=True)
    label_row = from_digits(arrived[:, piece : piece + 3].transpose(1, 0, 2)).reshape(total_tokens)

    prepared = packed_parts(table, group, groups)
    whole = spread(prepared, "dp")

    items = blocks * items_here
    item_columns = in_grad[0].reshape(items, groups, columns).transpose(1, 0, 2)
    lane = jnp.arange(64, dtype=jnp.int32)[None, :]
    marks = jnp.where(
        lane == 0,
        item_owner[0].reshape(items, 1),
        jnp.where(lane == 1, item_slot[0].reshape(items, 1) + 1, 0),
    ).astype(jnp.bfloat16)
    item_columns = jnp.concatenate(
        [item_columns, jnp.broadcast_to(marks[None], (groups, items, 64))], axis=2
    )
    item_columns = exchanged(item_columns, "dp")

    whole = assembled(whole, group, columns)
    raw = jnp.dot(whole, states, preferred_element_type=jnp.float32)
    squashed = jnp.tanh(raw * (1.0 / cap_value))
    capped = cap_value * squashed
    expd = jnp.exp(capped)
    row_ids = shard * rows + group * row_part + jnp.arange(row_part, dtype=jnp.int32)
    hits = row_ids[:, None] == label_row[None, :]
    local_total = jnp.sum(expd, axis=0)
    local_pick = jnp.sum(jnp.where(hits, capped, 0.0), axis=0)
    weights = (expd * (1.0 - squashed * squashed)).astype(jnp.bfloat16)
    local_sums = jnp.stack([local_total, local_pick])
    all_weights = lax.all_gather(weights, "dp", axis=0, tiled=True)

    sums = local_sums.reshape(-1, tokens)
    sums = sent_to_all(sums, "vocab").sum(axis=0)
    sums = sent_to_all(sums, "dp").sum(axis=0).reshape(2, total_tokens)
    total, picked = sums[0], sums[1]
    loss = lax.dynamic_slice(
        (jnp.log(total) - picked).reshape(groups, tokens), (group, 0), (1, tokens)
    )
    sent_rows = pack_items(item_columns, columns, groups * blocks, shards, capacity)
    got_rows = exchanged(sent_rows, "vocab").reshape(-1, columns + 64)
    targets = got_rows[:, columns + 1].astype(jnp.int32) - 1

    inverse = 1.0 / total
    label_weight = (
        (jnp.exp(picked) - total) * (1.0 - (picked / cap_value) ** 2)
    ).astype(jnp.bfloat16)
    shard_rows = shard * rows + jnp.arange(rows, dtype=jnp.int32)
    error = jnp.where(
        shard_rows[:, None] == label_row[None, :], label_weight[None, :], all_weights
    )

    partial_states = (
        lax.dot_general(
            table, error, (((0,), (0,)), ((), ())), preferred_element_type=jnp.float32
        )
        * inverse[None, :]
    ).astype(jnp.bfloat16)
    split = shards // groups
    parts = (
        partial_states.reshape(split, columns // split, groups, tokens)
        .transpose(2, 0, 1, 3)
        .reshape(shards, columns // split, tokens)
    )
    d_states = exchanged(parts, "vocab")
    d_states = d_states.astype(jnp.float32).sum(axis=0).astype(jnp.bfloat16)
    d_states = lax.ppermute(
        d_states,
        ("dp", "vocab"),
        [
            (z * shards + g * split + s, g * shards + z * split + s)
            for z in range(groups)
            for g in range(groups)
            for s in range(split)
        ],
    )
    d_hidden = d_states.T.reshape(1, blocks, span, columns // split)

    select = select_rows(new_mask, new_count)
    params = jnp.dot(select, table, preferred_element_type=jnp.float32)
    chosen = (
        jnp.dot(select, error, preferred_element_type=jnp.float32) * inverse[None, :]
    ).astype(jnp.bfloat16)
    own_states = lax.dynamic_slice(states, (group * columns, 0), (columns, total_tokens))
    grads = lax.dot_general(
        chosen, own_states, (((1,), (1,)), ((), ())), preferred_element_type=jnp.float32
    )
    picking = (jnp.arange(new_count, dtype=jnp.int32)[:, None] == targets[None, :]).astype(
        jnp.bfloat16
    )
    grads = grads + jnp.dot(
        picking, got_rows[:, :columns], preferred_element_type=jnp.float32
    )
    first_out = beta_one * first_moment + (1.0 - beta_one) * grads
    second_out = beta_two * second_moment + (1.0 - beta_two) * grads * grads
    update = (
        first_out
        / (1.0 - beta_one**step_count)
        / (jnp.sqrt(second_out / (1.0 - beta_two**step_count)) + epsilon)
        + decay_rate * params
    )
    return (loss.reshape(1, blocks, span), d_hidden, update, first_out, second_out)


def solution(mesh):
    return jax.shard_map(
        body,
        mesh=mesh,
        in_specs=(
            P("dp", None, None, None),
            P("vocab", "dp"),
            P("vocab"),
            P("dp", None, None),
            P("dp", None, "vocab", None),
            P("dp", None, "vocab", None),
            P("dp", None, "vocab"),
            P("vocab", "dp"),
            P("vocab", "dp"),
        ),
        out_specs=(
            P("dp", None, None),
            P("dp", None, None, "vocab"),
            P("vocab", "dp"),
            P("vocab", "dp"),
            P("vocab", "dp"),
        ),
        check_vma=False,
    )
```
